32 devices in a mesh: dp: 2 (over x), fsdp: 16 (over z, y, core).
Axes of the slice: x: 2, y: 2, z: 4, core: 2. Of those that a mesh axis runs over, the one named last changes fastest.
Arguments:
- small_cols: bfloat16 [24576, 128], P(('dp', 'fsdp')), may hold values from -6 to 6
- wide_cols: bfloat16 [24576, 2, 1536], P(('dp', 'fsdp')), may hold values from -24 to 24
- token_counts: int32 [32], P(('dp', 'fsdp')), may hold values from 144 to 768, as said below
- loss_sums: float32 [32], P(('dp', 'fsdp'))
- weight: float32 [128, 1536], P('fsdp'), may hold values from -0.75 to 0.75
- first_moment: float32 [128, 1536], P('fsdp'), may hold values from -0.002 to 0.002
- second_moment: float32 [128, 1536], P('fsdp'), may hold values from 1e-07 to 1e-06
- step: int32 [], replicated, may hold values from 1 to 2999
Outputs:
- new_weight: float32 [128, 1536], P('fsdp')
- new_first: float32 [128, 1536], P('fsdp')
- new_second: float32 [128, 1536], P('fsdp')
- adam_step: float32 [128, 1536], P('fsdp')
- grad_norm: float32 [], replicated
- mean_loss: float32 [], replicated
The draws below stay inside these ranges and needn't reach their ends.
Inputs may be any that keep to these rules, and one draw needn't show every extreme that they name: `token_counts`: each count is f * h * w with f from 1 to 3 and h, w from 12 to 16; in every draw some device's count is exactly 768.
All inputs are finite; a program needn't handle non-finite values.
Results may differ from the reference program's by a relative error of at most 0.0003.
Values sent between devices are 32-bit elements; how exact they have to be, the bound alone decides.
A program may use at most 64 MiB of HBM per device.

```python
import math
import jax
import jax.numpy as jnp
from jax import lax

D = 1536
PATCH = 64
FRAMES = 3
GRID = 16
CAP = 768
ROWS = 128
DEVS = 32


def draw_token_counts(key, part):
    keys = jax.random.split(jax.random.fold_in(key, 11), 4)
    frames = jax.random.randint(keys[0], (DEVS,), 1, FRAMES + 1)
    heights = jax.random.randint(keys[1], (DEVS,), 3 * GRID // 4, GRID + 1)
    widths = jax.random.randint(keys[2], (DEVS,), 3 * GRID // 4, GRID + 1)
    chosen = jax.random.randint(keys[3], (), 0, DEVS)
    counts = frames * heights * widths
    fullest = jnp.full((DEVS,), FRAMES * GRID * GRID, jnp.int32)
    return jnp.where(jnp.arange(DEVS) == chosen, fullest, counts).astype(jnp.int32)


def draw_loss_sums(key, part):
    keys = jax.random.split(jax.random.fold_in(key, 23), 1)
    ramp = 1.0 + 2.0 * jnp.arange(DEVS, dtype=jnp.float32) / max(DEVS - 1, 1)
    spread = jax.random.uniform(keys[0], (DEVS,), jnp.float32, 0.5, 1.5)
    values = 300.0 * ramp * spread
    return jnp.maximum(values, 10.0).astype(jnp.float32)


def with_spikes(drawn, own_key, source, target, parts, factor):
    def block_of(position):
        return (jnp.arange(drawn.shape[position]) // (drawn.shape[position] // parts)).reshape((-1,) + (1,) * (drawn.ndim - 1 - position))

    near = jax.random.permutation(own_key, parts)[block_of(target)]
    other_side = (block_of(target) + parts // 2) % parts
    return jnp.where((block_of(source) == near) | (block_of(source) == other_side), factor * drawn, drawn)


def steps_of(stream_key, shape, cuts, low, top_value):
    factor_of, own = 1.0, jax.random.fold_in(stream_key, 6)
    for axis_at, parts in cuts:
        steps = jnp.exp(jax.random.uniform(jax.random.fold_in(own, axis_at), (parts,), jnp.float32, low / len(cuts), top_value / len(cuts)))
        factor_of = factor_of * jnp.repeat(steps, shape[axis_at] // parts).reshape([-1 if axis == axis_at else 1 for axis in range(len(shape))])
    return factor_of


def gaussian(rng, dims, width, bound, cuts=(), held_as=jnp.bfloat16):
    drawn = width * jax.random.normal(rng, dims, jnp.float32)
    if cuts:
        drawn = drawn * steps_of(rng, dims, cuts, -0.22, 0.18)
    return jnp.clip(drawn, -bound, bound).astype(held_as)


def bell_draw_with(stream_key, extent, deviation, limit, cuts, heavy, kind=jnp.bfloat16):
    result = deviation * jax.random.normal(stream_key, extent, jnp.float32)
    if cuts:
        result = result * steps_of(stream_key, extent, cuts, -0.22, 0.18)
    return jnp.clip(with_spikes(result, jax.random.fold_in(stream_key, 3), *heavy), -limit, limit).astype(kind)


def setup_inputs(seed: int = 0) -> dict:
    splits = jax.random.split(jax.random.key(seed), 9)
    return {
        "small_cols": bell_draw_with(splits[0], (DEVS * CAP, ROWS), 1.0, 6.0, ((0, 32),), (0, 1, 32, 2.75)),
        "wide_cols": gaussian(splits[1], (DEVS * CAP, 2, D), 4.0, 24.0, ((0, 32),)),
        "token_counts": draw_token_counts(jax.random.fold_in(splits[8], 71), 0),
        "loss_sums": draw_loss_sums(jax.random.fold_in(splits[8], 71), 0),
        "weight": gaussian(splits[4], (ROWS, D), PATCH ** -0.5, 0.75, ((0, 16),), jnp.float32),
        "first_moment": gaussian(splits[5], (ROWS, D), 0.0003, 0.002, ((0, 16),), jnp.float32),
        "second_moment": jnp.clip(jnp.exp(math.log(9.999999974752427e-07) - 2.3025851 * jax.random.uniform(splits[6], (ROWS, D), jnp.float32) ** steps_of(splits[6], (ROWS, D), ((0, 16),), -0.2, 0.2)), 1.0000000116860974e-07, 9.999999974752427e-07),
        "step": jax.random.randint(splits[7], (), 1, 3000).astype(jnp.int32),
    }


MAX_NORM = 1.0
BETA_FIRST = 0.9
BETA_SECOND = 0.999
EPSILON_ADAM = 1e-08
LEARN_RATE = 0.02
DECAY_RATE = 0.1

def reference(small_cols, wide_cols, token_counts, loss_sums, weight, first_moment, second_moment, step):
    positions = jnp.arange(CAP, dtype=jnp.int32)

    def add_device(running, device):
        offset = (device * CAP).astype(jnp.int32)
        narrow = lax.dynamic_slice_in_dim(small_cols, offset, CAP, 0).astype(jnp.float32)
        broad = lax.dynamic_slice_in_dim(wide_cols, offset, CAP, 0).astype(jnp.float32)
        is_live = positions < token_counts[device]
        narrow = jnp.where(is_live[:, None], narrow, jnp.zeros_like(narrow))
        portion = jnp.einsum('thc,thd->hcd', narrow.reshape(CAP, 2, PATCH), broad)
        return (running + portion.reshape(ROWS, D), None)
    raw_sum, unused = lax.scan(add_device, jnp.zeros((ROWS, D), jnp.float32), jnp.arange(DEVS, dtype=jnp.int32))
    token_total = jnp.sum(token_counts.astype(jnp.float32))
    loss_total = jnp.sum(loss_sums)
    gradient = raw_sum / token_total
    grad_norm = jnp.sqrt(jnp.sum(gradient * gradient))
    mean_loss = loss_total / token_total
    clip_factor = jnp.minimum(1.0, MAX_NORM / (grad_norm + 1e-06))
    clipped = gradient * clip_factor
    new_first = BETA_FIRST * first_moment + (1.0 - BETA_FIRST) * clipped
    new_second = BETA_SECOND * second_moment + (1.0 - BETA_SECOND) * clipped * clipped
    step_float = step.astype(jnp.float32)
    first_hat = new_first / (1.0 - jnp.power(jnp.float32(BETA_FIRST), step_float))
    second_hat = new_second / (1.0 - jnp.power(jnp.float32(BETA_SECOND), step_float))
    adam_step = first_hat / (jnp.sqrt(second_hat) + EPSILON_ADAM) + DECAY_RATE * weight
    new_weight = weight - LEARN_RATE * adam_step
    return (new_weight, new_first, new_second, adam_step, grad_norm, mean_loss)
```

```python
import jax
import jax.numpy as jnp
from jax import lax
from jax.experimental import pallas as pl
from jax.experimental.pallas import tpu as pltpu
from jax.sharding import PartitionSpec as P
import functools

MAX_NORM = 1.0
BETA_FIRST = 0.9
BETA_SECOND = 0.999
EPSILON_ADAM = 1e-08
LEARN_RATE = 0.02
DECAY_RATE = 0.1


def slot_product(narrow, broad, live_count):
    block_rows = narrow.shape[0]
    half_cols = narrow.shape[1] // 2
    is_live = jnp.arange(block_rows, dtype=jnp.int32) < live_count
    narrow = jnp.where(is_live[:, None], narrow, jnp.zeros_like(narrow))
    portion = jnp.einsum(
        "thc,thd->hcd",
        narrow.reshape(block_rows, 2, half_cols),
        broad,
        preferred_element_type=jnp.float32,
    )
    return portion.reshape(2 * half_cols, broad.shape[2])


def device_term(small_cols, wide_cols, live_count):
    return slot_product(small_cols, wide_cols, live_count)


def on_device(
    small_cols, wide_cols, token_counts, loss_sums, weight, first_moment, second_moment, step
):
    live_count = token_counts[0]
    contribution = device_term(small_cols, wide_cols, live_count)
    count_float = token_counts.astype(jnp.float32)[0]
    loss_local = loss_sums[0]
    owned_sum = lax.psum_scatter(contribution, "fsdp", scatter_dimension=0, tiled=True)
    summed, count_groups, loss_groups = lax.psum((owned_sum, count_float, loss_local), "dp")
    squares, token_total, loss_total = lax.psum(
        (jnp.sum(summed * summed), count_groups, loss_groups), "fsdp"
    )
    gradient = summed / token_total
    grad_norm = jnp.sqrt(squares) / token_total
    mean_loss = loss_total / token_total
    clip_factor = jnp.minimum(1.0, MAX_NORM / (grad_norm + 1e-06))
    clipped = gradient * clip_factor
    new_first = BETA_FIRST * first_moment + (1.0 - BETA_FIRST) * clipped
    new_second = BETA_SECOND * second_moment + (1.0 - BETA_SECOND) * clipped * clipped
    step_float = step.astype(jnp.float32)
    first_hat = new_first / (1.0 - jnp.power(jnp.float32(BETA_FIRST), step_float))
    second_hat = new_second / (1.0 - jnp.power(jnp.float32(BETA_SECOND), step_float))
    adam_step = first_hat / (jnp.sqrt(second_hat) + EPSILON_ADAM) + DECAY_RATE * weight
    new_weight = weight - LEARN_RATE * adam_step
    return (new_weight, new_first, new_second, adam_step, grad_norm, mean_loss)


CORES = 2
SIDE = 2
LANES = 128
SUBLANES = 8
WIDTH = 2 * LANES
AHEAD = 2
MESH_ID = pl.DeviceIdType.MESH


def reduce_kernel(
    groups,
    owners,
    count_ref,
    loss_ref,
    narrow_hbm,
    broad_hbm,
    clipped_ref,
    stats_ref,
    narrow_buf,
    lhs_buf,
    broad_buf,
    own_buf,
    core_buf,
    chip_buf,
    plane_in,
    plane_sum,
    line_in,
    half_sum,
    half_in,
    stat_row,
    stat_in,
    narrow_sem,
    broad_sems,
    core_send,
    core_recv,
    plane_send,
    plane_recv,
    line_send,
    line_recv,
    half_send,
    half_recv,
    stat_send,
    stat_recv,
):
    slots, _, width = broad_hbm.shape
    line = owners // (CORES * SIDE)
    chunks = width // WIDTH
    per_half = chunks // groups
    devices = groups * owners
    dp = lax.axis_index("dp")
    place = lax.axis_index("fsdp")
    core = lax.rem(place, CORES)
    side = lax.rem(place // CORES, SIDE)
    level = place // (CORES * SIDE)
    me = dp * owners + place

    def place_of(level_at, side_at, core_at):
        return (level_at * SIDE + side_at) * CORES + core_at

    barrier = pltpu.get_barrier_semaphore()

    def greet(step, carry):
        other = lax.rem(me + step, devices)
        pl.semaphore_signal(
            barrier,
            inc=1,
            device_id=(other // owners, lax.rem(other, owners)),
            device_id_type=MESH_ID,
        )
        return carry

    lax.fori_loop(1, devices, greet, 0)

    narrow_copy = pltpu.make_async_copy(narrow_hbm, narrow_buf, narrow_sem)
    narrow_copy.start()

    def broad_copies(step):
        if step < per_half:
            chunk = (1 - dp) * per_half + step
        else:
            chunk = dp * per_half + step - per_half
        copies = []
        for part in range(2):
            column = pl.multiple_of(chunk * WIDTH + part * LANES, LANES)
            copies.append(
                pltpu.make_async_copy(
                    broad_hbm.at[:, :, pl.ds(column, LANES)],
                    broad_buf.at[2 * step + part],
                    broad_sems.at[2 * step + part],
                )
            )
        return copies

    for step in range(AHEAD):
        for copy in broad_copies(step):
            copy.start()

    live = count_ref[0]
    narrow_copy.wait()
    half_cols = narrow_hbm.shape[1] // 2
    slot_at = lax.broadcasted_iota(jnp.int32, (LANES, 2 * LANES), 0)
    pair_at = lax.broadcasted_iota(jnp.int32, (LANES, 2 * LANES), 1)
    spread = jnp.where(pair_at // 2 == slot_at, 1.0, 0.0).astype(jnp.bfloat16)
    in_half = lax.rem(pair_at, 2) == slot_at // half_cols
    for block in range(slots // LANES):
        doubled = lax.dot_general(
            narrow_buf[block * LANES : (block + 1) * LANES, :],
            spread,
            (((0,), (0,)), ((), ())),
            preferred_element_type=jnp.float32,
        )
        keep = in_half & (block * LANES + pair_at // 2 < live)
        lhs_buf[:, block * 2 * LANES : (block + 1) * 2 * LANES] = jnp.where(
            keep, doubled, 0.0
        ).astype(jnp.bfloat16)

    def core_copy(step):
        return pltpu.make_async_remote_copy(
            src_ref=own_buf.at[step, 1 - core],
            dst_ref=core_buf.at[step],
            send_sem=core_send.at[step],
            recv_sem=core_recv.at[step],
            device_id=(dp, place_of(level, side, 1 - core)),
            device_id_type=MESH_ID,
        )

    def plane_copy(slot, item):
        if slot == 2:
            source, side_to, dp_to = per_half + item, 1 - side, dp
        else:
            source, dp_to = item, 1 - dp
            side_to = side if slot == 0 else 1 - side
        return pltpu.make_async_remote_copy(
            src_ref=chip_buf.at[source, side_to],
            dst_ref=plane_in.at[slot, item],
            send_sem=plane_send.at[slot, item],
            recv_sem=plane_recv.at[slot, item],
            device_id=(dp_to, place_of(level, side_to, core)),
            device_id_type=MESH_ID,
        )

    def line_copy(hop, item):
        level_to = lax.rem(level + hop, line)
        return pltpu.make_async_remote_copy(
            src_ref=plane_sum.at[item, level_to],
            dst_ref=line_in.at[hop - 1, item],
            send_sem=line_send.at[hop - 1, item],
            recv_sem=line_recv.at[hop - 1, item],
            device_id=(dp, place_of(level_to, side, core)),
            device_id_type=MESH_ID,
        )

    def half_copy():
        return pltpu.make_async_remote_copy(
            src_ref=half_sum,
            dst_ref=half_in,
            send_sem=half_send,
            recv_sem=half_recv,
            device_id=(1 - dp, place),
            device_id_type=MESH_ID,
        )

    def stat_copy(step):
        other = lax.rem(me + step, devices)
        return pltpu.make_async_remote_copy(
            src_ref=stat_row,
            dst_ref=stat_in.at[step],
            send_sem=stat_send.at[step],
            recv_sem=stat_recv.at[step],
            device_id=(other // owners, lax.rem(other, owners)),
            device_id_type=MESH_ID,
        )

    def across_chip(step):
        core_copy(step).wait_recv()
        chip_buf[step] = own_buf[step, core] + core_buf[step]
        if step < per_half:
            plane_copy(1, step).start()
            plane_copy(0, step).start()
        else:
            plane_copy(2, step - per_half).start()

    lag = 2
    for step in range(chunks):
        if step + AHEAD < chunks:
            for copy in broad_copies(step + AHEAD):
                copy.start()
        for copy in broad_copies(step):
            copy.wait()
        block = jnp.concatenate(
            [
                broad_buf.at[2 * step + part].reshape(2 * slots, LANES)[...]
                for part in range(2)
            ],
            axis=1,
        )
        product = jnp.dot(lhs_buf[...], block, preferred_element_type=jnp.float32)
        for owner in range(owners):
            own_buf[
                step, owner % CORES, owner // CORES % SIDE, owner // (CORES * SIDE)
            ] = product[owner * SUBLANES : (owner + 1) * SUBLANES, :]
        if step == 0:
            pl.semaphore_wait(barrier, devices - 1)
        core_copy(step).start()
        if step >= lag:
            across_chip(step - lag)
    for step in range(chunks - lag, chunks):
        across_chip(step)

    for item in range(per_half):
        for slot in range(3):
            plane_copy(slot, item).wait_recv()
        plane_sum[item] = (
            chip_buf[per_half + item, side]
            + plane_in[0, item]
            + plane_in[1, item]
            + plane_in[2, item]
        )
        for hop in range(line - 1, 0, -1):
            line_copy(hop, item).start()

    squares = jnp.zeros((SUBLANES, WIDTH), jnp.float32)
    for item in range(per_half):
        total = plane_sum[item, level]
        for hop in range(1, line):
            line_copy(hop, item).wait_recv()
            total = total + line_in[hop - 1, item]
        half_sum[item] = total
        squares = squares + total * total
    lane = lax.broadcasted_iota(jnp.int32, (1, LANES), 1)
    row = jnp.where(
        lane == 0,
        jnp.sum(squares),
        jnp.where(
            lane == 1,
            live.astype(jnp.float32),
            jnp.where(lane == 2, loss_ref[0], 0.0),
        ),
    )
    stat_row[...] = row
    stat_in[0] = row

    def send_stat(step, carry):
        stat_copy(step).start()
        return carry

    half_copy().start()
    lax.fori_loop(1, devices, send_stat, 0)

    def drain_stat(step, carry):
        stat_copy(step).wait()
        return carry

    for step in range(chunks):
        core_copy(step).wait_send()
    for item in range(per_half):
        for slot in range(3):
            plane_copy(slot, item).wait_send()
        for hop in range(1, line):
            line_copy(hop, item).wait_send()
    half_copy().wait()
    lax.fori_loop(1, devices, drain_stat, 0)

    sums = jnp.sum(stat_in[...], axis=0)

    def entry(index):
        return jnp.sum(jnp.where(lane == index, sums, 0.0), axis=1, keepdims=True)

    token_total = entry(1)
    grad_norm = jnp.sqrt(entry(0)) / token_total
    mean_loss = entry(2) / token_total
    clip_factor = jnp.minimum(1.0, MAX_NORM / (grad_norm + 1e-06))
    for item in range(per_half):
        mine = pl.multiple_of((dp * per_half + item) * WIDTH, WIDTH)
        other = pl.multiple_of(((1 - dp) * per_half + item) * WIDTH, WIDTH)
        clipped_ref[:, pl.ds(mine, WIDTH)] = half_sum[item] / token_total * clip_factor
        clipped_ref[:, pl.ds(other, WIDTH)] = half_in[item] / token_total * clip_factor
    stats_ref[...] = jnp.where(lane == 0, grad_norm, mean_loss)


def reduce_clip(groups, owners, small_cols, wide_cols, token_counts, loss_sums):
    slots, _, width = wide_cols.shape
    line = owners // (CORES * SIDE)
    chunks = width // WIDTH
    per_half = chunks // groups
    tile = (SUBLANES, WIDTH)
    dma = pltpu.SemaphoreType.DMA
    return pl.pallas_call(
        functools.partial(reduce_kernel, groups, owners),
        out_shape=(
            jax.ShapeDtypeStruct((SUBLANES, width), jnp.float32),
            jax.ShapeDtypeStruct((1, LANES), jnp.float32),
        ),
        in_specs=[
            pl.BlockSpec(memory_space=pltpu.SMEM),
            pl.BlockSpec(memory_space=pltpu.SMEM),
            pl.BlockSpec(memory_space=pl.ANY),
            pl.BlockSpec(memory_space=pl.ANY),
        ],
        out_specs=(
            pl.BlockSpec(memory_space=pltpu.VMEM),
            pl.BlockSpec(memory_space=pltpu.VMEM),
        ),
        scratch_shapes=[
            pltpu.VMEM(small_cols.shape, jnp.bfloat16),
            pltpu.VMEM((small_cols.shape[1], 2 * slots), jnp.bfloat16),
            pltpu.VMEM((width // LANES, slots, 2, LANES), jnp.bfloat16),
            pltpu.VMEM((chunks, CORES, SIDE, line) + tile, jnp.float32),
            pltpu.VMEM((chunks, SIDE, line) + tile, jnp.float32),
            pltpu.VMEM((chunks, SIDE, line) + tile, jnp.float32),
            pltpu.VMEM((3, per_half, line) + tile, jnp.float32),
            pltpu.VMEM((per_half, line) + tile, jnp.float32),
            pltpu.VMEM((line - 1, per_half) + tile, jnp.float32),
            pltpu.VMEM((per_half,) + tile, jnp.float32),
            pltpu.VMEM((per_half,) + tile, jnp.float32),
            pltpu.VMEM((1, LANES), jnp.float32),
            pltpu.VMEM((groups * owners, 1, LANES), jnp.float32),
            dma,
            dma((width // LANES,)),
            dma((chunks,)),
            dma((chunks,)),
            dma((3, per_half)),
            dma((3, per_half)),
            dma((line - 1, per_half)),
            dma((line - 1, per_half)),
            dma,
            dma,
            dma((groups * owners,)),
            dma((groups * owners,)),
        ],
        compiler_params=pltpu.CompilerParams(collective_id=0, has_side_effects=True),
    )(token_counts, loss_sums, small_cols, wide_cols)


def on_device_kernel(
    groups,
    owners,
    small_cols,
    wide_cols,
    token_counts,
    loss_sums,
    weight,
    first_moment,
    second_moment,
    step,
):
    clipped, stats = reduce_clip(
        groups, owners, small_cols, wide_cols, token_counts, loss_sums
    )
    new_first = BETA_FIRST * first_moment + (1.0 - BETA_FIRST) * clipped
    new_second = BETA_SECOND * second_moment + (1.0 - BETA_SECOND) * clipped * clipped
    step_float = step.astype(jnp.float32)
    first_hat = new_first / (1.0 - jnp.power(jnp.float32(BETA_FIRST), step_float))
    second_hat = new_second / (1.0 - jnp.power(jnp.float32(BETA_SECOND), step_float))
    adam_step = first_hat / (jnp.sqrt(second_hat) + EPSILON_ADAM) + DECAY_RATE * weight
    new_weight = weight - LEARN_RATE * adam_step
    return (new_weight, new_first, new_second, adam_step, stats[0, 0], stats[0, 1])


def solution(mesh):
    in_specs = (
        P(("dp", "fsdp"), None),
        P(("dp", "fsdp"), None, None),
        P(("dp", "fsdp")),
        P(("dp", "fsdp")),
        P("fsdp", None),
        P("fsdp", None),
        P("fsdp", None),
        P(),
    )
    out_specs = (P("fsdp", None), P("fsdp", None), P("fsdp", None), P("fsdp", None), P(), P())
    groups, owners = mesh.shape["dp"], mesh.shape["fsdp"]

    def step_fn(small_cols, *rest):
        rows = small_cols.shape[1]
        fits = groups == SIDE and owners * SUBLANES == rows
        body = functools.partial(on_device_kernel, groups, owners) if fits else on_device
        return jax.shard_map(
            body, mesh=mesh, in_specs=in_specs, out_specs=out_specs, check_vma=False
        )(small_cols, *rest)

    return step_fn
```

```python
import jax
import jax.numpy as jnp
from jax import lax
from jax.experimental import pallas as pl
from jax.experimental.pallas import tpu as pltpu
from jax.sharding import PartitionSpec as P
import functools

MAX_NORM = 1.0
BETA_FIRST = 0.9
BETA_SECOND = 0.999
EPSILON_ADAM = 1e-08
LEARN_RATE = 0.02
DECAY_RATE = 0.1


def slot_product(narrow, broad, live_count):
    block_rows = narrow.shape[0]
    half_cols = narrow.shape[1] // 2
    is_live = jnp.arange(block_rows, dtype=jnp.int32) < live_count
    narrow = jnp.where(is_live[:, None], narrow, jnp.zeros_like(narrow))
    portion = jnp.einsum(
        "thc,thd->hcd",
        narrow.reshape(block_rows, 2, half_cols),
        broad,
        preferred_element_type=jnp.float32,
    )
    return portion.reshape(2 * half_cols, broad.shape[2])


def device_term(small_cols, wide_cols, live_count):
    return slot_product(small_cols, wide_cols, live_count)


def on_device(
    small_cols, wide_cols, token_counts, loss_sums, weight, first_moment, second_moment, step
):
    live_count = token_counts[0]
    contribution = device_term(small_cols, wide_cols, live_count)
    count_float = token_counts.astype(jnp.float32)[0]
    loss_local = loss_sums[0]
    owned_sum = lax.psum_scatter(contribution, "fsdp", scatter_dimension=0, tiled=True)
    summed, count_groups, loss_groups = lax.psum((owned_sum, count_float, loss_local), "dp")
    squares, token_total, loss_total = lax.psum(
        (jnp.sum(summed * summed), count_groups, loss_groups), "fsdp"
    )
    gradient = summed / token_total
    grad_norm = jnp.sqrt(squares) / token_total
    mean_loss = loss_total / token_total
    clip_factor = jnp.minimum(1.0, MAX_NORM / (grad_norm + 1e-06))
    clipped = gradient * clip_factor
    new_first = BETA_FIRST * first_moment + (1.0 - BETA_FIRST) * clipped
    new_second = BETA_SECOND * second_moment + (1.0 - BETA_SECOND) * clipped * clipped
    step_float = step.astype(jnp.float32)
    first_hat = new_first / (1.0 - jnp.power(jnp.float32(BETA_FIRST), step_float))
    second_hat = new_second / (1.0 - jnp.power(jnp.float32(BETA_SECOND), step_float))
    adam_step = first_hat / (jnp.sqrt(second_hat) + EPSILON_ADAM) + DECAY_RATE * weight
    new_weight = weight - LEARN_RATE * adam_step
    return (new_weight, new_first, new_second, adam_step, grad_norm, mean_loss)


CORES = 2
SIDE = 2
LANES = 128
SUBLANES = 8
WIDTH = 2 * LANES
AHEAD = 2
STEP_BITS = 16
MESH_ID = pl.DeviceIdType.MESH


def complement_power(base, exponent):
    square = 1.0 - jnp.float32(base)
    total = jnp.float32(0.0)
    for bit in range(STEP_BITS):
        taken = (exponent // (1 << bit)) % 2 == 1
        total = jnp.where(taken, total + square - total * square, total)
        square = square * (2.0 - square)
    return total


def reduce_kernel(
    groups,
    owners,
    narrow_hbm,
    broad_hbm,
    count_hbm,
    loss_hbm,
    weight_hbm,
    first_hbm,
    second_hbm,
    step_hbm,
    weight_out,
    first_out,
    second_out,
    adam_out,
    norm_out,
    loss_out,
    count_ref,
    loss_ref,
    step_ref,
    weight_buf,
    first_buf,
    second_buf,
    narrow_buf,
    lhs_buf,
    broad_buf,
    own_buf,
    core_buf,
    chip_buf,
    plane_in,
    plane_sum,
    line_in,
    half_sum,
    half_in,
    stat_row,
    stat_in,
    small_sems,
    broad_sems,
    core_send,
    core_recv,
    plane_send,
    plane_recv,
    line_send,
    line_recv,
    half_send,
    half_recv,
    stat_send,
    stat_recv,
):
    slots, _, width = broad_hbm.shape
    line = owners // (CORES * SIDE)
    chunks = width // WIDTH
    per_half = chunks // groups
    devices = groups * owners
    dp = lax.axis_index("dp")
    place = lax.axis_index("fsdp")
    core = lax.rem(place, CORES)
    side = lax.rem(place // CORES, SIDE)
    level = place // (CORES * SIDE)
    me = dp * owners + place

    def place_of(level_at, side_at, core_at):
        return (level_at * SIDE + side_at) * CORES + core_at

    barrier = pltpu.get_barrier_semaphore()

    partners = [(dp, place_of(level, side, 1 - core))]
    partners += [
        (1 - dp, place),
        (1 - dp, place_of(level, 1 - side, core)),
        (dp, place_of(level, 1 - side, core)),
    ]
    for hop in range(1, line):
        partners.append((dp, place_of(lax.rem(level + hop, line), side, core)))
    for partner in partners:
        pl.semaphore_signal(
            barrier, inc=1, device_id=partner, device_id_type=MESH_ID
        )

    narrow_copy = pltpu.make_async_copy(narrow_hbm, narrow_buf, small_sems.at[0])
    count_copy = pltpu.make_async_copy(count_hbm, count_ref, small_sems.at[1])
    late_copies = [
        pltpu.make_async_copy(loss_hbm, loss_ref, small_sems.at[2]),
        pltpu.make_async_copy(step_hbm, step_ref, small_sems.at[3]),
        pltpu.make_async_copy(weight_hbm, weight_buf, small_sems.at[4]),
        pltpu.make_async_copy(first_hbm, first_buf, small_sems.at[5]),
        pltpu.make_async_copy(second_hbm, second_buf, small_sems.at[6]),
    ]
    narrow_copy.start()
    count_copy.start()

    def broad_copies(step):
        if step < per_half:
            chunk = (1 - dp) * per_half + step
        else:
            chunk = dp * per_half + step - per_half
        copies = []
        for part in range(2):
            column = pl.multiple_of(chunk * WIDTH + part * LANES, LANES)
            copies.append(
                pltpu.make_async_copy(
                    broad_hbm.at[:, :, pl.ds(column, LANES)],
                    broad_buf.at[2 * step + part],
                    broad_sems.at[2 * step + part],
                )
            )
        return copies

    for step in range(AHEAD):
        for copy in broad_copies(step):
            copy.start()

    count_copy.wait()
    live = count_ref[0, 0]
    narrow_copy.wait()
    half_cols = narrow_hbm.shape[1] // 2
    slot_at = lax.broadcasted_iota(jnp.int32, (LANES, 2 * LANES), 0)
    pair_at = lax.broadcasted_iota(jnp.int32, (LANES, 2 * LANES), 1)
    spread = jnp.where(pair_at // 2 == slot_at, 1.0, 0.0).astype(jnp.bfloat16)
    in_half = lax.rem(pair_at, 2) == slot_at // half_cols
    for block in range(slots // LANES):
        doubled = lax.dot_general(
            narrow_buf[block * LANES : (block + 1) * LANES, :],
            spread,
            (((0,), (0,)), ((), ())),
            preferred_element_type=jnp.float32,
        )
        keep = in_half & (block * LANES + pair_at // 2 < live)
        lhs_buf[:, block * 2 * LANES : (block + 1) * 2 * LANES] = jnp.where(
            keep, doubled, 0.0
        ).astype(jnp.bfloat16)

    def core_copy(step):
        return pltpu.make_async_remote_copy(
            src_ref=own_buf.at[step, 1 - core],
            dst_ref=core_buf.at[step],
            send_sem=core_send.at[step],
            recv_sem=core_recv.at[step],
            device_id=(dp, place_of(level, side, 1 - core)),
            device_id_type=MESH_ID,
        )

    def plane_copy(slot, item):
        if slot == 2:
            source, side_to, dp_to = per_half + item, 1 - side, dp
        else:
            source, dp_to = item, 1 - dp
            side_to = side if slot == 0 else 1 - side
        return pltpu.make_async_remote_copy(
            src_ref=chip_buf.at[source, side_to],
            dst_ref=plane_in.at[slot, item],
            send_sem=plane_send.at[slot, item],
            recv_sem=plane_recv.at[slot, item],
            device_id=(dp_to, place_of(level, side_to, core)),
            device_id_type=MESH_ID,
        )

    def line_copy(hop, item):
        level_to = lax.rem(level + hop, line)
        return pltpu.make_async_remote_copy(
            src_ref=plane_sum.at[item, level_to],
            dst_ref=line_in.at[hop - 1, item],
            send_sem=line_send.at[hop - 1, item],
            recv_sem=line_recv.at[hop - 1, item],
            device_id=(dp, place_of(level_to, side, core)),
            device_id_type=MESH_ID,
        )

    def half_copy():
        return pltpu.make_async_remote_copy(
            src_ref=half_sum,
            dst_ref=half_in,
            send_sem=half_send,
            recv_sem=half_recv,
            device_id=(1 - dp, place),
            device_id_type=MESH_ID,
        )

    def stat_copy(step):
        other = lax.rem(me + step, devices)
        return pltpu.make_async_remote_copy(
            src_ref=stat_row,
            dst_ref=stat_in.at[step],
            send_sem=stat_send.at[step],
            recv_sem=stat_recv.at[step],
            device_id=(other // owners, lax.rem(other, owners)),
            device_id_type=MESH_ID,
        )

    def across_chip(step):
        core_copy(step).wait_recv()
        chip_buf[step] = own_buf[step, core] + core_buf[step]
        if step < per_half:
            plane_copy(1, step).start()
            plane_copy(0, step).start()
        else:
            plane_copy(2, step - per_half).start()

    lag = 2
    for copy in late_copies:
        copy.start()
    for step in range(chunks):
        if step + AHEAD < chunks:
            for copy in broad_copies(step + AHEAD):
                copy.start()
        for copy in broad_copies(step):
            copy.wait()
        block = jnp.concatenate(
            [
                broad_buf.at[2 * step + part].reshape(2 * slots, LANES)[...]
                for part in range(2)
            ],
            axis=1,
        )
        product = jnp.dot(lhs_buf[...], block, preferred_element_type=jnp.float32)
        for owner in range(owners):
            own_buf[
                step, owner % CORES, owner // CORES % SIDE, owner // (CORES * SIDE)
            ] = product[owner * SUBLANES : (owner + 1) * SUBLANES, :]
        if step == 0:
            pl.semaphore_wait(barrier, len(partners))
        core_copy(step).start()
        if step >= lag:
            across_chip(step - lag)
    for step in range(chunks - lag, chunks):
        across_chip(step)
    for copy in late_copies:
        copy.wait()

    for item in range(per_half):
        for slot in range(3):
            plane_copy(slot, item).wait_recv()
        plane_sum[item] = (
            chip_buf[per_half + item, side]
            + plane_in[0, item]
            + plane_in[1, item]
            + plane_in[2, item]
        )
        for hop in range(line - 1, 0, -1):
            line_copy(hop, item).start()

    squares = jnp.zeros((SUBLANES, WIDTH), jnp.float32)
    for item in range(per_half):
        total = plane_sum[item, level]
        for hop in range(1, line):
            line_copy(hop, item).wait_recv()
            total = total + line_in[hop - 1, item]
        half_sum[item] = total
        squares = squares + total * total
    lane = lax.broadcasted_iota(jnp.int32, (1, LANES), 1)
    row = jnp.where(
        lane == 0,
        jnp.sum(squares),
        jnp.where(
            lane == 1,
            live.astype(jnp.float32),
            jnp.where(lane == 2, loss_ref[0, 0], 0.0),
        ),
    )
    stat_row[...] = row
    stat_in[0] = row

    def send_stat(step, carry):
        stat_copy(step).start()
        return carry

    half_copy().start()
    lax.fori_loop(1, devices, send_stat, 0)

    def drain_stat(step, carry):
        stat_copy(step).wait()
        return carry

    first_fix = complement_power(BETA_FIRST, step_ref[0, 0])
    second_fix = complement_power(BETA_SECOND, step_ref[0, 0])
    for step in range(chunks):
        core_copy(step).wait_send()
    for item in range(per_half):
        for slot in range(3):
            plane_copy(slot, item).wait_send()
        for hop in range(1, line):
            line_copy(hop, item).wait_send()
    half_copy().wait()
    lax.fori_loop(1, devices, drain_stat, 0)

    sums = jnp.sum(stat_in[...], axis=0)

    def entry(index):
        return jnp.sum(jnp.where(lane == index, sums, 0.0), axis=1, keepdims=True)

    token_total = entry(1)
    grad_norm = jnp.sqrt(entry(0)) / token_total
    mean_loss = entry(2) / token_total
    clip_factor = jnp.minimum(1.0, MAX_NORM / (grad_norm + 1e-06))
    for item in range(per_half):
        for source, half in ((half_sum, dp), (half_in, 1 - dp)):
            columns = pl.ds(
                pl.multiple_of((half * per_half + item) * WIDTH, WIDTH), WIDTH
            )
            clipped = source[item] / token_total * clip_factor
            new_first = (
                BETA_FIRST * first_buf[:, columns] + (1.0 - BETA_FIRST) * clipped
            )
            new_second = (
                BETA_SECOND * second_buf[:, columns]
                + (1.0 - BETA_SECOND) * clipped * clipped
            )
            first_hat = new_first / first_fix
            second_hat = new_second / second_fix
            weight = weight_buf[:, columns]
            adam_step = (
                first_hat / (jnp.sqrt(second_hat) + EPSILON_ADAM) + DECAY_RATE * weight
            )
            first_out[:, columns] = new_first
            second_out[:, columns] = new_second
            adam_out[:, columns] = adam_step
            weight_out[:, columns] = weight - LEARN_RATE * adam_step
    norm_out[...] = grad_norm
    loss_out[...] = mean_loss


def write_kernel(*refs):
    count = len(refs) // 2
    sems = refs[-1]
    copies = [
        pltpu.make_async_copy(refs[at], refs[count + at], sems.at[at])
        for at in range(count)
    ]
    for copy in copies:
        copy.start()
    for copy in copies:
        copy.wait()


def on_device_kernel(
    groups,
    owners,
    small_cols,
    wide_cols,
    token_counts,
    loss_sums,
    weight,
    first_moment,
    second_moment,
    step,
):
    slots, _, width = wide_cols.shape
    line = owners // (CORES * SIDE)
    chunks = width // WIDTH
    per_half = chunks // groups
    tile = (SUBLANES, WIDTH)
    dma = pltpu.SemaphoreType.DMA
    shapes = [weight.shape] * 4 + [(1, 1)] * 2
    in_vmem = pl.BlockSpec(memory_space=pltpu.VMEM)
    anywhere = pl.BlockSpec(memory_space=pl.ANY)
    results = pl.pallas_call(
        functools.partial(reduce_kernel, groups, owners),
        out_shape=[pltpu.VMEM(shape, jnp.float32) for shape in shapes],
        in_specs=[pl.BlockSpec(memory_space=pltpu.HBM)] * 8,
        out_specs=[in_vmem] * len(shapes),
        scratch_shapes=[
            pltpu.SMEM((1, 1), jnp.int32),
            pltpu.SMEM((1, 1), jnp.float32),
            pltpu.SMEM((1, 1), jnp.int32),
            pltpu.VMEM(weight.shape, jnp.float32),
            pltpu.VMEM(weight.shape, jnp.float32),
            pltpu.VMEM(weight.shape, jnp.float32),
            pltpu.VMEM(small_cols.shape, jnp.bfloat16),
            pltpu.VMEM((small_cols.shape[1], 2 * slots), jnp.bfloat16),
            pltpu.VMEM((width // LANES, slots, 2, LANES), jnp.bfloat16),
            pltpu.VMEM((chunks, CORES, SIDE, line) + tile, jnp.float32),
            pltpu.VMEM((chunks, SIDE, line) + tile, jnp.float32),
            pltpu.VMEM((chunks, SIDE, line) + tile, jnp.float32),
            pltpu.VMEM((3, per_half, line) + tile, jnp.float32),
            pltpu.VMEM((per_half, line) + tile, jnp.float32),
            pltpu.VMEM((line - 1, per_half) + tile, jnp.float32),
            pltpu.VMEM((per_half,) + tile, jnp.float32),
            pltpu.VMEM((per_half,) + tile, jnp.float32),
            pltpu.VMEM((1, LANES), jnp.float32),
            pltpu.VMEM((groups * owners, 1, LANES), jnp.float32),
            dma((7,)),
            dma((width // LANES,)),
            dma((chunks,)),
            dma((chunks,)),
            dma((3, per_half)),
            dma((3, per_half)),
            dma((line - 1, per_half)),
            dma((line - 1, per_half)),
            dma,
            dma,
            dma((groups * owners,)),
            dma((groups * owners,)),
        ],
        compiler_params=pltpu.CompilerParams(collective_id=0, has_side_effects=True),
    )(
        small_cols,
        wide_cols,
        token_counts.reshape(1, 1),
        loss_sums.reshape(1, 1),
        weight,
        first_moment,
        second_moment,
        step.reshape(1, 1),
    )
    outputs = pl.pallas_call(
        write_kernel,
        out_shape=[jax.ShapeDtypeStruct(shape, jnp.float32) for shape in shapes],
        in_specs=[anywhere] * len(shapes),
        out_specs=[anywhere] * len(shapes),
        scratch_shapes=[dma((len(shapes),))],
    )(*[pltpu.with_memory_space_constraint(result, pltpu.VMEM) for result in results])
    return tuple(outputs[:4]) + (outputs[4][0, 0], outputs[5][0, 0])


def solution(mesh):
    in_specs = (
        P(("dp", "fsdp"), None),
        P(("dp", "fsdp"), None, None),
        P(("dp", "fsdp")),
        P(("dp", "fsdp")),
        P("fsdp", None),
        P("fsdp", None),
        P("fsdp", None),
        P(),
    )
    out_specs = (P("fsdp", None), P("fsdp", None), P("fsdp", None), P("fsdp", None), P(), P())
    groups, owners = mesh.shape["dp"], mesh.shape["fsdp"]

    def step_fn(small_cols, *rest):
        rows = small_cols.shape[1]
        fits = groups == SIDE and owners * SUBLANES == rows
        body = functools.partial(on_device_kernel, groups, owners) if fits else on_device
        return jax.shard_map(
            body, mesh=mesh, in_specs=in_specs, out_specs=out_specs, check_vma=False
        )(small_cols, *rest)

    return step_fn
```

```python
import jax
import jax.numpy as jnp
from jax import lax
from jax.experimental import pallas as pl
from jax.experimental.pallas import tpu as pltpu
from jax.sharding import PartitionSpec as P
import functools

MAX_NORM = 1.0
BETA_FIRST = 0.9
BETA_SECOND = 0.999
EPSILON_ADAM = 1e-08
LEARN_RATE = 0.02
DECAY_RATE = 0.1


def slot_product(narrow, broad, live_count):
    block_rows = narrow.shape[0]
    half_cols = narrow.shape[1] // 2
    is_live = jnp.arange(block_rows, dtype=jnp.int32) < live_count
    narrow = jnp.where(is_live[:, None], narrow, jnp.zeros_like(narrow))
    portion = jnp.einsum(
        "thc,thd->hcd",
        narrow.reshape(block_rows, 2, half_cols),
        broad,
        preferred_element_type=jnp.float32,
    )
    return portion.reshape(2 * half_cols, broad.shape[2])


def device_term(small_cols, wide_cols, live_count):
    return slot_product(small_cols, wide_cols, live_count)


def on_device(
    small_cols, wide_cols, token_counts, loss_sums, weight, first_moment, second_moment, step
):
    live_count = token_counts[0]
    contribution = device_term(small_cols, wide_cols, live_count)
    count_float = token_counts.astype(jnp.float32)[0]
    loss_local = loss_sums[0]
    owned_sum = lax.psum_scatter(contribution, "fsdp", scatter_dimension=0, tiled=True)
    summed, count_groups, loss_groups = lax.psum((owned_sum, count_float, loss_local), "dp")
    squares, token_total, loss_total = lax.psum(
        (jnp.sum(summed * summed), count_groups, loss_groups), "fsdp"
    )
    gradient = summed / token_total
    grad_norm = jnp.sqrt(squares) / token_total
    mean_loss = loss_total / token_total
    clip_factor = jnp.minimum(1.0, MAX_NORM / (grad_norm + 1e-06))
    clipped = gradient * clip_factor
    new_first = BETA_FIRST * first_moment + (1.0 - BETA_FIRST) * clipped
    new_second = BETA_SECOND * second_moment + (1.0 - BETA_SECOND) * clipped * clipped
    step_float = step.astype(jnp.float32)
    first_hat = new_first / (1.0 - jnp.power(jnp.float32(BETA_FIRST), step_float))
    second_hat = new_second / (1.0 - jnp.power(jnp.float32(BETA_SECOND), step_float))
    adam_step = first_hat / (jnp.sqrt(second_hat) + EPSILON_ADAM) + DECAY_RATE * weight
    new_weight = weight - LEARN_RATE * adam_step
    return (new_weight, new_first, new_second, adam_step, grad_norm, mean_loss)


CORES = 2
SIDE = 2
LANES = 128
SUBLANES = 8
WIDTH = 2 * LANES
AHEAD = 2
STEP_BITS = 16
MESH_ID = pl.DeviceIdType.MESH


def complement_power(base, exponent):
    square = 1.0 - jnp.float32(base)
    total = jnp.float32(0.0)
    for bit in range(STEP_BITS):
        taken = (exponent // (1 << bit)) % 2 == 1
        total = jnp.where(taken, total + square - total * square, total)
        square = square * (2.0 - square)
    return total


def reduce_kernel(
    groups,
    owners,
    narrow_hbm,
    broad_hbm,
    count_hbm,
    loss_hbm,
    weight_hbm,
    first_hbm,
    second_hbm,
    step_hbm,
    weight_out,
    first_out,
    second_out,
    adam_out,
    norm_out,
    loss_out,
    count_ref,
    loss_ref,
    step_ref,
    weight_buf,
    first_buf,
    second_buf,
    narrow_buf,
    lhs_buf,
    broad_buf,
    own_buf,
    core_buf,
    chip_buf,
    plane_in,
    plane_sum,
    line_in,
    early_in,
    early_sum,
    early_plane,
    half_sum,
    half_in,
    stat_row,
    stat_in,
    small_sems,
    broad_sems,
    core_send,
    core_recv,
    plane_send,
    plane_recv,
    line_send,
    line_recv,
    early_send,
    early_recv,
    half_send,
    half_recv,
    stat_send,
    stat_recv,
):
    slots, _, width = broad_hbm.shape
    line = owners // (CORES * SIDE)
    chunks = width // WIDTH
    per_half = chunks // groups
    devices = groups * owners
    dp = lax.axis_index("dp")
    place = lax.axis_index("fsdp")
    core = lax.rem(place, CORES)
    side = lax.rem(place // CORES, SIDE)
    level = place // (CORES * SIDE)
    me = dp * owners + place

    def place_of(level_at, side_at, core_at):
        return (level_at * SIDE + side_at) * CORES + core_at

    barrier = pltpu.get_barrier_semaphore()

    partners = [(dp, place_of(level, side, 1 - core))]
    partners += [
        (1 - dp, place),
        (1 - dp, place_of(level, 1 - side, core)),
        (dp, place_of(level, 1 - side, core)),
    ]
    for hop in range(1, line):
        partners.append((dp, place_of(lax.rem(level + hop, line), side, core)))
    for partner in partners:
        pl.semaphore_signal(
            barrier, inc=1, device_id=partner, device_id_type=MESH_ID
        )

    narrow_copy = pltpu.make_async_copy(narrow_hbm, narrow_buf, small_sems.at[0])
    count_copy = pltpu.make_async_copy(count_hbm, count_ref, small_sems.at[1])
    late_copies = [
        pltpu.make_async_copy(loss_hbm, loss_ref, small_sems.at[2]),
        pltpu.make_async_copy(step_hbm, step_ref, small_sems.at[3]),
        pltpu.make_async_copy(weight_hbm, weight_buf, small_sems.at[4]),
        pltpu.make_async_copy(first_hbm, first_buf, small_sems.at[5]),
        pltpu.make_async_copy(second_hbm, second_buf, small_sems.at[6]),
    ]
    narrow_copy.start()
    count_copy.start()

    def broad_copies(step):
        if step < per_half:
            chunk = (1 - dp) * per_half + step
        else:
            chunk = dp * per_half + step - per_half
        copies = []
        for part in range(2):
            column = pl.multiple_of(chunk * WIDTH + part * LANES, LANES)
            copies.append(
                pltpu.make_async_copy(
                    broad_hbm.at[:, :, pl.ds(column, LANES)],
                    broad_buf.at[2 * step + part],
                    broad_sems.at[2 * step + part],
                )
            )
        return copies

    for step in sorted(range(0, chunks, per_half))[:AHEAD]:
        for copy in broad_copies(step):
            copy.start()

    count_copy.wait()
    live = count_ref[0, 0]
    narrow_copy.wait()
    half_cols = narrow_hbm.shape[1] // 2
    slot_at = lax.broadcasted_iota(jnp.int32, (LANES, 2 * LANES), 0)
    pair_at = lax.broadcasted_iota(jnp.int32, (LANES, 2 * LANES), 1)
    spread = jnp.where(pair_at // 2 == slot_at, 1.0, 0.0).astype(jnp.bfloat16)
    in_half = lax.rem(pair_at, 2) == slot_at // half_cols
    for block in range(slots // LANES):
        doubled = lax.dot_general(
            narrow_buf[block * LANES : (block + 1) * LANES, :],
            spread,
            (((0,), (0,)), ((), ())),
            preferred_element_type=jnp.float32,
        )
        keep = in_half & (block * LANES + pair_at // 2 < live)
        lhs_buf[:, block * 2 * LANES : (block + 1) * 2 * LANES] = jnp.where(
            keep, doubled, 0.0
        ).astype(jnp.bfloat16)

    def core_copy(step):
        return pltpu.make_async_remote_copy(
            src_ref=own_buf.at[step, 1 - core],
            dst_ref=core_buf.at[step],
            send_sem=core_send.at[step],
            recv_sem=core_recv.at[step],
            device_id=(dp, place_of(level, side, 1 - core)),
            device_id_type=MESH_ID,
        )

    def plane_copy(slot, item):
        if slot == 2:
            source, side_to, dp_to = per_half + item, 1 - side, dp
        else:
            source, dp_to = item, 1 - dp
            side_to = side if slot == 0 else 1 - side
        return pltpu.make_async_remote_copy(
            src_ref=early_sum.at[source // per_half, side_to]
            if item == 0
            else chip_buf.at[source, side_to],
            dst_ref=early_plane.at[slot] if item == 0 else plane_in.at[slot, item],
            send_sem=plane_send.at[slot, item],
            recv_sem=plane_recv.at[slot, item],
            device_id=(dp_to, place_of(level, side_to, core)),
            device_id_type=MESH_ID,
        )

    def line_copy(hop, item):
        level_to = lax.rem(level + hop, line)
        return pltpu.make_async_remote_copy(
            src_ref=plane_sum.at[item, level_to],
            dst_ref=line_in.at[hop - 1, item],
            send_sem=line_send.at[hop - 1, item],
            recv_sem=line_recv.at[hop - 1, item],
            device_id=(dp, place_of(level_to, side, core)),
            device_id_type=MESH_ID,
        )

    def early_copy(hop, half):
        level_to = lax.rem(level + hop, line)
        return pltpu.make_async_remote_copy(
            src_ref=chip_buf.at[half * per_half, :, level_to],
            dst_ref=early_in.at[hop - 1, half],
            send_sem=early_send.at[hop - 1, half],
            recv_sem=early_recv.at[hop - 1, half],
            device_id=(dp, place_of(level_to, side, core)),
            device_id_type=MESH_ID,
        )

    def half_copy():
        return pltpu.make_async_remote_copy(
            src_ref=half_sum,
            dst_ref=half_in,
            send_sem=half_send,
            recv_sem=half_recv,
            device_id=(1 - dp, place),
            device_id_type=MESH_ID,
        )

    def stat_copy(step):
        other = lax.rem(me + step, devices)
        return pltpu.make_async_remote_copy(
            src_ref=stat_row,
            dst_ref=stat_in.at[step],
            send_sem=stat_send.at[step],
            recv_sem=stat_recv.at[step],
            device_id=(other // owners, lax.rem(other, owners)),
            device_id_type=MESH_ID,
        )

    def across_chip(step):
        core_copy(step).wait_recv()
        chip_buf[step] = own_buf[step, core] + core_buf[step]
        if step % per_half == 0:
            for hop in range(line - 1, 0, -1):
                early_copy(hop, step // per_half).start()
        elif step < per_half:
            plane_copy(1, step).start()
            plane_copy(0, step).start()
        else:
            plane_copy(2, step - per_half).start()

    lag = 2
    order = sorted(range(chunks), key=lambda at: (at % per_half != 0, at))
    for copy in late_copies:
        copy.start()
    for at, step in enumerate(order):
        if at + AHEAD < chunks:
            for copy in broad_copies(order[at + AHEAD]):
                copy.start()
        for copy in broad_copies(step):
            copy.wait()
        block = jnp.concatenate(
            [
                broad_buf.at[2 * step + part].reshape(2 * slots, LANES)[...]
                for part in range(2)
            ],
            axis=1,
        )
        product = jnp.dot(lhs_buf[...], block, preferred_element_type=jnp.float32)
        for owner in range(owners):
            own_buf[
                step, owner % CORES, owner // CORES % SIDE, owner // (CORES * SIDE)
            ] = product[owner * SUBLANES : (owner + 1) * SUBLANES, :]
        if at == 0:
            pl.semaphore_wait(barrier, len(partners))
        core_copy(step).start()
        if at >= lag:
            across_chip(order[at - lag])
    for step in order[chunks - lag :]:
        across_chip(step)
    for copy in late_copies:
        copy.wait()

    for half in range(groups):
        gathered = chip_buf[half * per_half, :, level]
        for hop in range(1, line):
            early_copy(hop, half).wait_recv()
            gathered = gathered + early_in[hop - 1, half]
        early_sum[half] = gathered
    for slot in (1, 0, 2):
        plane_copy(slot, 0).start()
    for item in range(1, per_half):
        for slot in range(3):
            plane_copy(slot, item).wait_recv()
        plane_sum[item] = (
            chip_buf[per_half + item, side]
            + plane_in[0, item]
            + plane_in[1, item]
            + plane_in[2, item]
        )
        for hop in range(line - 1, 0, -1):
            line_copy(hop, item).start()

    squares = jnp.zeros((SUBLANES, WIDTH), jnp.float32)
    for item in range(per_half):
        if item == 0:
            total = early_sum[1, side]
            for slot in range(3):
                plane_copy(slot, item).wait_recv()
                total = total + early_plane[slot]
        else:
            total = plane_sum[item, level]
            for hop in range(1, line):
                line_copy(hop, item).wait_recv()
                total = total + line_in[hop - 1, item]
        half_sum[item] = total
        squares = squares + total * total
    lane = lax.broadcasted_iota(jnp.int32, (1, LANES), 1)
    row = jnp.where(
        lane == 0,
        jnp.sum(squares),
        jnp.where(
            lane == 1,
            live.astype(jnp.float32),
            jnp.where(lane == 2, loss_ref[0, 0], 0.0),
        ),
    )
    stat_row[...] = row
    stat_in[0] = row

    def send_stat(step, carry):
        stat_copy(step).start()
        return carry

    half_copy().start()
    lax.fori_loop(1, devices, send_stat, 0)

    def drain_stat(step, carry):
        stat_copy(step).wait()
        return carry

    first_fix = complement_power(BETA_FIRST, step_ref[0, 0])
    second_fix = complement_power(BETA_SECOND, step_ref[0, 0])
    for step in range(chunks):
        core_copy(step).wait_send()
    for item in range(per_half):
        for slot in range(3):
            plane_copy(slot, item).wait_send()
        for hop in range(1, line):
            if item > 0:
                line_copy(hop, item).wait_send()
            if item < groups:
                early_copy(hop, item).wait_send()
    half_copy().wait()
    lax.fori_loop(1, devices, drain_stat, 0)

    sums = jnp.sum(stat_in[...], axis=0)

    def entry(index):
        return jnp.sum(jnp.where(lane == index, sums, 0.0), axis=1, keepdims=True)

    token_total = entry(1)
    grad_norm = jnp.sqrt(entry(0)) / token_total
    mean_loss = entry(2) / token_total
    clip_factor = jnp.minimum(1.0, MAX_NORM / (grad_norm + 1e-06))
    for item in range(per_half):
        for source, half in ((half_sum, dp), (half_in, 1 - dp)):
            columns = pl.ds(
                pl.multiple_of((half * per_half + item) * WIDTH, WIDTH), WIDTH
            )
            clipped = source[item] / token_total * clip_factor
            new_first = (
                BETA_FIRST * first_buf[:, columns] + (1.0 - BETA_FIRST) * clipped
            )
            new_second = (
                BETA_SECOND * second_buf[:, columns]
                + (1.0 - BETA_SECOND) * clipped * clipped
            )
            first_hat = new_first / first_fix
            second_hat = new_second / second_fix
            weight = weight_buf[:, columns]
            adam_step = (
                first_hat / (jnp.sqrt(second_hat) + EPSILON_ADAM) + DECAY_RATE * weight
            )
            first_out[:, columns] = new_first
            second_out[:, columns] = new_second
            adam_out[:, columns] = adam_step
            weight_out[:, columns] = weight - LEARN_RATE * adam_step
    norm_out[...] = grad_norm
    loss_out[...] = mean_loss


def write_kernel(*refs):
    count = len(refs) // 2
    sems = refs[-1]
    copies = [
        pltpu.make_async_copy(refs[at], refs[count + at], sems.at[at])
        for at in range(count)
    ]
    for copy in copies:
        copy.start()
    for copy in copies:
        copy.wait()


def on_device_kernel(
    groups,
    owners,
    small_cols,
    wide_cols,
    token_counts,
    loss_sums,
    weight,
    first_moment,
    second_moment,
    step,
):
    slots, _, width = wide_cols.shape
    line = owners // (CORES * SIDE)
    chunks = width // WIDTH
    per_half = chunks // groups
    tile = (SUBLANES, WIDTH)
    dma = pltpu.SemaphoreType.DMA
    shapes = [weight.shape] * 4 + [(1, 1)] * 2
    in_vmem = pl.BlockSpec(memory_space=pltpu.VMEM)
    anywhere = pl.BlockSpec(memory_space=pl.ANY)
    results = pl.pallas_call(
        functools.partial(reduce_kernel, groups, owners),
        out_shape=[pltpu.VMEM(shape, jnp.float32) for shape in shapes],
        in_specs=[pl.BlockSpec(memory_space=pltpu.HBM)] * 8,
        out_specs=[in_vmem] * len(shapes),
        scratch_shapes=[
            pltpu.SMEM((1, 1), jnp.int32),
            pltpu.SMEM((1, 1), jnp.float32),
            pltpu.SMEM((1, 1), jnp.int32),
            pltpu.VMEM(weight.shape, jnp.float32),
            pltpu.VMEM(weight.shape, jnp.float32),
            pltpu.VMEM(weight.shape, jnp.float32),
            pltpu.VMEM(small_cols.shape, jnp.bfloat16),
            pltpu.VMEM((small_cols.shape[1], 2 * slots), jnp.bfloat16),
            pltpu.VMEM((width // LANES, slots, 2, LANES), jnp.bfloat16),
            pltpu.VMEM((chunks, CORES, SIDE, line) + tile, jnp.float32),
            pltpu.VMEM((chunks, SIDE, line) + tile, jnp.float32),
            pltpu.VMEM((chunks, SIDE, line) + tile, jnp.float32),
            pltpu.VMEM((3, per_half, line) + tile, jnp.float32),
            pltpu.VMEM((per_half, line) + tile, jnp.float32),
            pltpu.VMEM((line - 1, per_half) + tile, jnp.float32),
            pltpu.VMEM((line - 1, groups, SIDE) + tile, jnp.float32),
            pltpu.VMEM((groups, SIDE) + tile, jnp.float32),
            pltpu.VMEM((3,) + tile, jnp.float32),
            pltpu.VMEM((per_half,) + tile, jnp.float32),
            pltpu.VMEM((per_half,) + tile, jnp.float32),
            pltpu.VMEM((1, LANES), jnp.float32),
            pltpu.VMEM((groups * owners, 1, LANES), jnp.float32),
            dma((7,)),
            dma((width // LANES,)),
            dma((chunks,)),
            dma((chunks,)),
            dma((3, per_half)),
            dma((3, per_half)),
            dma((line - 1, per_half)),
            dma((line - 1, per_half)),
            dma((line - 1, groups)),
            dma((line - 1, groups)),
            dma,
            dma,
            dma((groups * owners,)),
            dma((groups * owners,)),
        ],
        compiler_params=pltpu.CompilerParams(collective_id=0, has_side_effects=True),
    )(
        small_cols,
        wide_cols,
        token_counts.reshape(1, 1),
        loss_sums.reshape(1, 1),
        weight,
        first_moment,
        second_moment,
        step.reshape(1, 1),
    )
    outputs = pl.pallas_call(
        write_kernel,
        out_shape=[jax.ShapeDtypeStruct(shape, jnp.float32) for shape in shapes],
        in_specs=[anywhere] * len(shapes),
        out_specs=[anywhere] * len(shapes),
        scratch_shapes=[dma((len(shapes),))],
    )(*[pltpu.with_memory_space_constraint(result, pltpu.VMEM) for result in results])
    return tuple(outputs[:4]) + (outputs[4][0, 0], outputs[5][0, 0])


def solution(mesh):
    in_specs = (
        P(("dp", "fsdp"), None),
        P(("dp", "fsdp"), None, None),
        P(("dp", "fsdp")),
        P(("dp", "fsdp")),
        P("fsdp", None),
        P("fsdp", None),
        P("fsdp", None),
        P(),
    )
    out_specs = (P("fsdp", None), P("fsdp", None), P("fsdp", None), P("fsdp", None), P(), P())
    groups, owners = mesh.shape["dp"], mesh.shape["fsdp"]

    def step_fn(small_cols, *rest):
        rows = small_cols.shape[1]
        fits = groups == SIDE and owners * SUBLANES == rows
        body = functools.partial(on_device_kernel, groups, owners) if fits else on_device
        return jax.shard_map(
            body, mesh=mesh, in_specs=in_specs, out_specs=out_specs, check_vma=False
        )(small_cols, *rest)

    return step_fn
```

```python
import jax
import jax.numpy as jnp
from jax import lax
from jax.experimental import pallas as pl
from jax.experimental.pallas import tpu as pltpu
from jax.sharding import PartitionSpec as P
import functools

MAX_NORM = 1.0
BETA_FIRST = 0.9
BETA_SECOND = 0.999
EPSILON_ADAM = 1e-08
LEARN_RATE = 0.02
DECAY_RATE = 0.1


def slot_product(narrow, broad, live_count):
    block_rows = narrow.shape[0]
    half_cols = narrow.shape[1] // 2
    is_live = jnp.arange(block_rows, dtype=jnp.int32) < live_count
    narrow = jnp.where(is_live[:, None], narrow, jnp.zeros_like(narrow))
    portion = jnp.einsum(
        "thc,thd->hcd",
        narrow.reshape(block_rows, 2, half_cols),
        broad,
        preferred_element_type=jnp.float32,
    )
    return portion.reshape(2 * half_cols, broad.shape[2])


def device_term(small_cols, wide_cols, live_count):
    return slot_product(small_cols, wide_cols, live_count)


def on_device(
    small_cols, wide_cols, token_counts, loss_sums, weight, first_moment, second_moment, step
):
    live_count = token_counts[0]
    contribution = device_term(small_cols, wide_cols, live_count)
    count_float = token_counts.astype(jnp.float32)[0]
    loss_local = loss_sums[0]
    owned_sum = lax.psum_scatter(contribution, "fsdp", scatter_dimension=0, tiled=True)
    summed, count_groups, loss_groups = lax.psum((owned_sum, count_float, loss_local), "dp")
    squares, token_total, loss_total = lax.psum(
        (jnp.sum(summed * summed), count_groups, loss_groups), "fsdp"
    )
    gradient = summed / token_total
    grad_norm = jnp.sqrt(squares) / token_total
    mean_loss = loss_total / token_total
    clip_factor = jnp.minimum(1.0, MAX_NORM / (grad_norm + 1e-06))
    clipped = gradient * clip_factor
    new_first = BETA_FIRST * first_moment + (1.0 - BETA_FIRST) * clipped
    new_second = BETA_SECOND * second_moment + (1.0 - BETA_SECOND) * clipped * clipped
    step_float = step.astype(jnp.float32)
    first_hat = new_first / (1.0 - jnp.power(jnp.float32(BETA_FIRST), step_float))
    second_hat = new_second / (1.0 - jnp.power(jnp.float32(BETA_SECOND), step_float))
    adam_step = first_hat / (jnp.sqrt(second_hat) + EPSILON_ADAM) + DECAY_RATE * weight
    new_weight = weight - LEARN_RATE * adam_step
    return (new_weight, new_first, new_second, adam_step, grad_norm, mean_loss)


CORES = 2
SIDE = 2
LANES = 128
SUBLANES = 8
WIDTH = 2 * LANES
AHEAD = 2
STEP_BITS = 16
MESH_ID = pl.DeviceIdType.MESH


def complement_power(base, exponent):
    square = 1.0 - jnp.float32(base)
    total = jnp.float32(0.0)
    for bit in range(STEP_BITS):
        taken = (exponent // (1 << bit)) % 2 == 1
        total = jnp.where(taken, total + square - total * square, total)
        square = square * (2.0 - square)
    return total


def reduce_kernel(
    groups,
    owners,
    narrow_hbm,
    broad_hbm,
    count_hbm,
    loss_hbm,
    weight_hbm,
    first_hbm,
    second_hbm,
    step_hbm,
    weight_out,
    first_out,
    second_out,
    adam_out,
    norm_out,
    loss_out,
    count_ref,
    loss_ref,
    step_ref,
    weight_buf,
    first_buf,
    second_buf,
    narrow_buf,
    lhs_buf,
    broad_buf,
    own_buf,
    core_buf,
    chip_buf,
    plane_in,
    plane_sum,
    line_in,
    early_in,
    early_sum,
    early_plane,
    half_sum,
    half_in,
    stat_row,
    stat_in,
    small_sems,
    broad_sems,
    core_send,
    core_recv,
    plane_send,
    plane_recv,
    line_send,
    line_recv,
    early_send,
    early_recv,
    half_send,
    half_recv,
    stat_send,
    stat_recv,
):
    slots, _, width = broad_hbm.shape
    line = owners // (CORES * SIDE)
    chunks = width // WIDTH
    per_half = chunks // groups
    devices = groups * owners
    dp = lax.axis_index("dp")
    place = lax.axis_index("fsdp")
    core = lax.rem(place, CORES)
    side = lax.rem(place // CORES, SIDE)
    level = place // (CORES * SIDE)
    me = dp * owners + place

    def place_of(level_at, side_at, core_at):
        return (level_at * SIDE + side_at) * CORES + core_at

    barrier = pltpu.get_barrier_semaphore()

    partners = [(dp, place_of(level, side, 1 - core))]
    partners += [
        (1 - dp, place),
        (1 - dp, place_of(level, 1 - side, core)),
        (dp, place_of(level, 1 - side, core)),
    ]
    for hop in range(1, line):
        partners.append((dp, place_of(lax.rem(level + hop, line), side, core)))
    for partner in partners:
        pl.semaphore_signal(
            barrier, inc=1, device_id=partner, device_id_type=MESH_ID
        )

    narrow_copy = pltpu.make_async_copy(narrow_hbm, narrow_buf, small_sems.at[0])
    count_copy = pltpu.make_async_copy(count_hbm, count_ref, small_sems.at[1])
    late_copies = [
        pltpu.make_async_copy(loss_hbm, loss_ref, small_sems.at[2]),
        pltpu.make_async_copy(step_hbm, step_ref, small_sems.at[3]),
        pltpu.make_async_copy(weight_hbm, weight_buf, small_sems.at[4]),
        pltpu.make_async_copy(first_hbm, first_buf, small_sems.at[5]),
        pltpu.make_async_copy(second_hbm, second_buf, small_sems.at[6]),
    ]
    narrow_copy.start()
    count_copy.start()

    def broad_copies(step):
        if step < per_half:
            chunk = (1 - dp) * per_half + step
        else:
            chunk = dp * per_half + step - per_half
        copies = []
        for part in range(2):
            column = pl.multiple_of(chunk * WIDTH + part * LANES, LANES)
            copies.append(
                pltpu.make_async_copy(
                    broad_hbm.at[:, :, pl.ds(column, LANES)],
                    broad_buf.at[2 * step + part],
                    broad_sems.at[2 * step + part],
                )
            )
        return copies

    for step in sorted(range(0, chunks, per_half))[:AHEAD]:
        for copy in broad_copies(step):
            copy.start()

    count_copy.wait()
    live = count_ref[0, 0]
    narrow_copy.wait()
    half_cols = narrow_hbm.shape[1] // 2
    slot_at = lax.broadcasted_iota(jnp.int32, (LANES, 2 * LANES), 0)
    pair_at = lax.broadcasted_iota(jnp.int32, (LANES, 2 * LANES), 1)
    spread = jnp.where(pair_at // 2 == slot_at, 1.0, 0.0).astype(jnp.bfloat16)
    in_half = lax.rem(pair_at, 2) == slot_at // half_cols
    for block in range(slots // LANES):
        doubled = lax.dot_general(
            narrow_buf[block * LANES : (block + 1) * LANES, :],
            spread,
            (((0,), (0,)), ((), ())),
            preferred_element_type=jnp.float32,
        )
        keep = in_half & (block * LANES + pair_at // 2 < live)
        lhs_buf[:, block * 2 * LANES : (block + 1) * 2 * LANES] = jnp.where(
            keep, doubled, 0.0
        ).astype(jnp.bfloat16)

    def core_copy(step):
        return pltpu.make_async_remote_copy(
            src_ref=own_buf.at[step, 1 - core],
            dst_ref=core_buf.at[step],
            send_sem=core_send.at[step],
            recv_sem=core_recv.at[step],
            device_id=(dp, place_of(level, side, 1 - core)),
            device_id_type=MESH_ID,
        )

    def plane_copy(slot, item):
        if slot == 2:
            source, side_to, dp_to = per_half + item, 1 - side, dp
        else:
            source, dp_to = item, 1 - dp
            side_to = side if slot == 0 else 1 - side
        return pltpu.make_async_remote_copy(
            src_ref=early_sum.at[source // per_half, side_to]
            if item == 0
            else chip_buf.at[source, side_to],
            dst_ref=early_plane.at[slot] if item == 0 else plane_in.at[slot, item],
            send_sem=plane_send.at[slot, item],
            recv_sem=plane_recv.at[slot, item],
            device_id=(dp_to, place_of(level, side_to, core)),
            device_id_type=MESH_ID,
        )

    def line_copy(hop, item):
        level_to = lax.rem(level + hop, line)
        return pltpu.make_async_remote_copy(
            src_ref=plane_sum.at[item, level_to],
            dst_ref=line_in.at[hop - 1, item],
            send_sem=line_send.at[hop - 1, item],
            recv_sem=line_recv.at[hop - 1, item],
            device_id=(dp, place_of(level_to, side, core)),
            device_id_type=MESH_ID,
        )

    def early_copy(hop, half):
        level_to = lax.rem(level + hop, line)
        return pltpu.make_async_remote_copy(
            src_ref=chip_buf.at[half * per_half, :, level_to],
            dst_ref=early_in.at[hop - 1, half],
            send_sem=early_send.at[hop - 1, half],
            recv_sem=early_recv.at[hop - 1, half],
            device_id=(dp, place_of(level_to, side, core)),
            device_id_type=MESH_ID,
        )

    def half_copy():
        return pltpu.make_async_remote_copy(
            src_ref=half_sum,
            dst_ref=half_in,
            send_sem=half_send,
            recv_sem=half_recv,
            device_id=(1 - dp, place),
            device_id_type=MESH_ID,
        )

    def stat_copy(step):
        other = lax.rem(me + step, devices)
        return pltpu.make_async_remote_copy(
            src_ref=stat_row,
            dst_ref=stat_in.at[step],
            send_sem=stat_send.at[step],
            recv_sem=stat_recv.at[step],
            device_id=(other // owners, lax.rem(other, owners)),
            device_id_type=MESH_ID,
        )

    def across_chip(step):
        core_copy(step).wait_recv()
        chip_buf[step] = own_buf[step, core] + core_buf[step]
        if step % per_half == 0:
            for hop in range(line - 1, 0, -1):
                early_copy(hop, step // per_half).start()
        elif step < per_half:
            plane_copy(1, step).start()
            plane_copy(0, step).start()
        else:
            plane_copy(2, step - per_half).start()

    lag = 1
    order = sorted(range(chunks), key=lambda at: (at % per_half != 0, at))
    for copy in late_copies:
        copy.start()
    for at, step in enumerate(order):
        if at + AHEAD < chunks:
            for copy in broad_copies(order[at + AHEAD]):
                copy.start()
        for copy in broad_copies(step):
            copy.wait()
        block = jnp.concatenate(
            [
                broad_buf.at[2 * step + part].reshape(2 * slots, LANES)[...]
                for part in range(2)
            ],
            axis=1,
        )
        product = jnp.dot(lhs_buf[...], block, preferred_element_type=jnp.float32)
        for owner in range(owners):
            own_buf[
                step, owner % CORES, owner // CORES % SIDE, owner // (CORES * SIDE)
            ] = product[owner * SUBLANES : (owner + 1) * SUBLANES, :]
        if at == 0:
            pl.semaphore_wait(barrier, len(partners))
        core_copy(step).start()
        if at >= lag:
            across_chip(order[at - lag])
    for step in order[chunks - lag :]:
        across_chip(step)
    for copy in late_copies:
        copy.wait()

    for half in range(groups):
        gathered = chip_buf[half * per_half, :, level]
        for hop in range(1, line):
            early_copy(hop, half).wait_recv()
            gathered = gathered + early_in[hop - 1, half]
        early_sum[half] = gathered
    for slot in (1, 0, 2):
        plane_copy(slot, 0).start()
    for item in range(1, per_half):
        for slot in range(3):
            plane_copy(slot, item).wait_recv()
        plane_sum[item] = (
            chip_buf[per_half + item, side]
            + plane_in[0, item]
            + plane_in[1, item]
            + plane_in[2, item]
        )
        for hop in range(line - 1, 0, -1):
            line_copy(hop, item).start()

    squares = jnp.zeros((SUBLANES, WIDTH), jnp.float32)
    for item in range(per_half):
        if item == 0:
            total = early_sum[1, side]
            for slot in range(3):
                plane_copy(slot, item).wait_recv()
                total = total + early_plane[slot]
        else:
            total = plane_sum[item, level]
            for hop in range(1, line):
                line_copy(hop, item).wait_recv()
                total = total + line_in[hop - 1, item]
        half_sum[item] = total
        squares = squares + total * total
    lane = lax.broadcasted_iota(jnp.int32, (1, LANES), 1)
    row = jnp.where(
        lane == 0,
        jnp.sum(squares),
        jnp.where(
            lane == 1,
            live.astype(jnp.float32),
            jnp.where(lane == 2, loss_ref[0, 0], 0.0),
        ),
    )
    stat_row[...] = row
    stat_in[0] = row

    def send_stat(step, carry):
        stat_copy(step).start()
        return carry

    half_copy().start()
    lax.fori_loop(1, devices, send_stat, 0)

    def drain_stat(step, carry):
        stat_copy(step).wait()
        return carry

    first_fix = complement_power(BETA_FIRST, step_ref[0, 0])
    second_fix = complement_power(BETA_SECOND, step_ref[0, 0])
    for step in range(chunks):
        core_copy(step).wait_send()
    for item in range(per_half):
        for slot in range(3):
            plane_copy(slot, item).wait_send()
        for hop in range(1, line):
            if item > 0:
                line_copy(hop, item).wait_send()
            if item < groups:
                early_copy(hop, item).wait_send()
    half_copy().wait()
    lax.fori_loop(1, devices, drain_stat, 0)

    sums = jnp.sum(stat_in[...], axis=0)

    def entry(index):
        return jnp.sum(jnp.where(lane == index, sums, 0.0), axis=1, keepdims=True)

    token_total = entry(1)
    grad_norm = jnp.sqrt(entry(0)) / token_total
    mean_loss = entry(2) / token_total
    clip_factor = jnp.minimum(1.0, MAX_NORM / (grad_norm + 1e-06))
    for item in range(per_half):
        for source, half in ((half_sum, dp), (half_in, 1 - dp)):
            columns = pl.ds(
                pl.multiple_of((half * per_half + item) * WIDTH, WIDTH), WIDTH
            )
            clipped = source[item] / token_total * clip_factor
            new_first = (
                BETA_FIRST * first_buf[:, columns] + (1.0 - BETA_FIRST) * clipped
            )
            new_second = (
                BETA_SECOND * second_buf[:, columns]
                + (1.0 - BETA_SECOND) * clipped * clipped
            )
            first_hat = new_first / first_fix
            second_hat = new_second / second_fix
            weight = weight_buf[:, columns]
            adam_step = (
                first_hat / (jnp.sqrt(second_hat) + EPSILON_ADAM) + DECAY_RATE * weight
            )
            first_out[:, columns] = new_first
            second_out[:, columns] = new_second
            adam_out[:, columns] = adam_step
            weight_out[:, columns] = weight - LEARN_RATE * adam_step
    norm_out[...] = grad_norm
    loss_out[...] = mean_loss


def write_kernel(*refs):
    count = len(refs) // 2
    sems = refs[-1]
    copies = [
        pltpu.make_async_copy(refs[at], refs[count + at], sems.at[at])
        for at in range(count)
    ]
    for copy in copies:
        copy.start()
    for copy in copies:
        copy.wait()


def on_device_kernel(
    groups,
    owners,
    small_cols,
    wide_cols,
    token_counts,
    loss_sums,
    weight,
    first_moment,
    second_moment,
    step,
):
    slots, _, width = wide_cols.shape
    line = owners // (CORES * SIDE)
    chunks = width // WIDTH
    per_half = chunks // groups
    tile = (SUBLANES, WIDTH)
    dma = pltpu.SemaphoreType.DMA
    shapes = [weight.shape] * 4 + [(1, 1)] * 2
    in_vmem = pl.BlockSpec(memory_space=pltpu.VMEM)
    anywhere = pl.BlockSpec(memory_space=pl.ANY)
    results = pl.pallas_call(
        functools.partial(reduce_kernel, groups, owners),
        out_shape=[pltpu.VMEM(shape, jnp.float32) for shape in shapes],
        in_specs=[pl.BlockSpec(memory_space=pltpu.HBM)] * 8,
        out_specs=[in_vmem] * len(shapes),
        scratch_shapes=[
            pltpu.SMEM((1, 1), jnp.int32),
            pltpu.SMEM((1, 1), jnp.float32),
            pltpu.SMEM((1, 1), jnp.int32),
            pltpu.VMEM(weight.shape, jnp.float32),
            pltpu.VMEM(weight.shape, jnp.float32),
            pltpu.VMEM(weight.shape, jnp.float32),
            pltpu.VMEM(small_cols.shape, jnp.bfloat16),
            pltpu.VMEM((small_cols.shape[1], 2 * slots), jnp.bfloat16),
            pltpu.VMEM((width // LANES, slots, 2, LANES), jnp.bfloat16),
            pltpu.VMEM((chunks, CORES, SIDE, line) + tile, jnp.float32),
            pltpu.VMEM((chunks, SIDE, line) + tile, jnp.float32),
            pltpu.VMEM((chunks, SIDE, line) + tile, jnp.float32),
            pltpu.VMEM((3, per_half, line) + tile, jnp.float32),
            pltpu.VMEM((per_half, line) + tile, jnp.float32),
            pltpu.VMEM((line - 1, per_half) + tile, jnp.float32),
            pltpu.VMEM((line - 1, groups, SIDE) + tile, jnp.float32),
            pltpu.VMEM((groups, SIDE) + tile, jnp.float32),
            pltpu.VMEM((3,) + tile, jnp.float32),
            pltpu.VMEM((per_half,) + tile, jnp.float32),
            pltpu.VMEM((per_half,) + tile, jnp.float32),
            pltpu.VMEM((1, LANES), jnp.float32),
            pltpu.VMEM((groups * owners, 1, LANES), jnp.float32),
            dma((7,)),
            dma((width // LANES,)),
            dma((chunks,)),
            dma((chunks,)),
            dma((3, per_half)),
            dma((3, per_half)),
            dma((line - 1, per_half)),
            dma((line - 1, per_half)),
            dma((line - 1, groups)),
            dma((line - 1, groups)),
            dma,
            dma,
            dma((groups * owners,)),
            dma((groups * owners,)),
        ],
        compiler_params=pltpu.CompilerParams(collective_id=0, has_side_effects=True),
    )(
        small_cols,
        wide_cols,
        token_counts.reshape(1, 1),
        loss_sums.reshape(1, 1),
        weight,
        first_moment,
        second_moment,
        step.reshape(1, 1),
    )
    outputs = pl.pallas_call(
        write_kernel,
        out_shape=[jax.ShapeDtypeStruct(shape, jnp.float32) for shape in shapes],
        in_specs=[anywhere] * len(shapes),
        out_specs=[anywhere] * len(shapes),
        scratch_shapes=[dma((len(shapes),))],
    )(*[pltpu.with_memory_space_constraint(result, pltpu.VMEM) for result in results])
    return tuple(outputs[:4]) + (outputs[4][0, 0], outputs[5][0, 0])


def solution(mesh):
    in_specs = (
        P(("dp", "fsdp"), None),
        P(("dp", "fsdp"), None, None),
        P(("dp", "fsdp")),
        P(("dp", "fsdp")),
        P("fsdp", None),
        P("fsdp", None),
        P("fsdp", None),
        P(),
    )
    out_specs = (P("fsdp", None), P("fsdp", None), P("fsdp", None), P("fsdp", None), P(), P())
    groups, owners = mesh.shape["dp"], mesh.shape["fsdp"]

    def step_fn(small_cols, *rest):
        rows = small_cols.shape[1]
        fits = groups == SIDE and owners * SUBLANES == rows
        body = functools.partial(on_device_kernel, groups, owners) if fits else on_device
        return jax.shard_map(
            body, mesh=mesh, in_specs=in_specs, out_specs=out_specs, check_vma=False
        )(small_cols, *rest)

    return step_fn
```
